32 devices in a mesh: groups: 2 (over y), blk: 4 (over z), heads: 2 (over x), beam: 2 (over core).
Axes of the slice: x: 2, y: 2, z: 4, core: 2. Of those that a mesh axis runs over, the one named last changes fastest.
Arguments:
- queries: bfloat16 [4, 32, 64, 128], P(('groups', 'beam'), 'blk', 'heads'), parts along dimension 0, may hold values from -110 to 110
- positions: int32 [4, 32], P(('groups', 'beam'), 'blk'), parts along dimension 0, may hold values from 512 to 4096
- row_order: int32 [4, 32], P(('groups', 'beam')), parts along dimension 0, may hold values from 0 to 31, each once within a row
- lengths: int32 [8], P(('groups', 'blk')), parts along dimension 0, may hold values from 128 to 1024
- cache_keys: bfloat16 [8, 4, 1024, 128], P(('groups', 'blk'), 'heads'), parts along dimension 0, may hold values from -4 to 4
- cache_values: bfloat16 [8, 4, 1024, 128], P(('groups', 'blk'), 'heads'), parts along dimension 0, may hold values from -6 to 6
Outputs:
- attended: bfloat16 [4, 32, 64, 128], P(('groups', 'beam'), 'blk', 'heads'), parts along dimension 0
The draws below stay inside these ranges and needn't reach their ends.
There are 2 independent parts, one for each index of `groups`. The reference program is written for one: setup_inputs(seed, part) draws one part's arguments, and reference() takes and returns one part's arrays. A program takes and returns all parts, laid end to end along the dimension named above; each array names one. Nothing has to cross between parts.
Inputs may be any that keep to these rules, and one draw needn't show every extreme that they name: Slots of shard s from lengths[s] on hold no cache entry. `positions`: a row reads the cache entries whose global position, counted shard after shard as in the reference program, lies below its position. row_order[e] is a permutation of 0 to 31.
All inputs are finite; a program needn't handle non-finite values.
Results may differ from the reference program's by a relative error of at most 0.0015.
Values may be sent and summed in bfloat16 or wider, within the bound.
A program may use at most 64 MiB of HBM per device.

```python
import math
import jax
import jax.numpy as jnp
from jax import lax

HQ = 64
KVH = 4
HD = 128
CAP = 1024
KB = 256
GQ = 16
SETS = 2
SHARDS = 4
ROWS_SET = 32
CONTEXT = 4096


def base_keys(key):
    drawn = jax.random.normal(jax.random.fold_in(key, 11), (SHARDS, KVH, CAP, HD), jnp.float32)
    drawn = jnp.clip(drawn, -4.0, 4.0)
    return drawn


def draw_cache_keys(key, part):
    return base_keys(key).astype(jnp.bfloat16)


def draw_queries(key, part):
    full_shape = (SETS, ROWS_SET, HQ, HD)
    scales = jnp.exp(jax.random.uniform(jax.random.fold_in(key, 26), (SETS, ROWS_SET, HQ, 1), jnp.float32, 0.0, math.log(12.0)))
    entries = jnp.clip(2.5 * scales * jax.random.normal(jax.random.fold_in(key, 25), full_shape, jnp.float32), -110.0, 110.0)
    return entries.astype(jnp.bfloat16)


def plant(values, key, low, largest):
    extent = values.shape
    index_at = [jax.random.randint(jax.random.fold_in(key, axis), (), 0, extent[axis]) for axis in range(len(extent))]
    values = values.at[tuple(index_at)].set(low)
    longest = extent.index(max(extent))
    index_at[longest] = (index_at[longest] + 1) % extent[longest]
    return values.at[tuple(index_at)].set(largest)


def levels(rng, shape, pieces, low, high):
    factor_of = 1.0
    for axis_at, blocks in pieces:
        draws = jax.random.uniform(jax.random.fold_in(jax.random.fold_in(rng, 6), axis_at), (blocks,), jnp.float32, low / len(pieces), high / len(pieces))
        factor_of = factor_of * jnp.repeat(jnp.exp(draws), shape[axis_at] // blocks).reshape((-1,) + (1,) * (len(shape) - 1 - axis_at))
    return factor_of


def bell_draw(rng, dims, width, reach, pieces=(), kind=jnp.bfloat16):
    level = levels(rng, dims, pieces, -0.22, 0.18) if pieces else 1.0
    values = jax.random.normal(rng, dims, jnp.float32) * width * level
    return jnp.minimum(jnp.maximum(values, -reach), reach).astype(kind)


def setup_inputs(seed: int = 0, part: int = 0) -> dict:
    key_list = jax.random.split(jax.random.key(seed), 7)
    own_keys = jax.random.split(jax.random.fold_in(key_list[6], part), 7)
    return {
        "queries": draw_queries(jax.random.fold_in(jax.random.fold_in(key_list[6], part), 71), part),
        "positions": plant(jax.random.randint(own_keys[1], (SETS, ROWS_SET), CONTEXT // 8, CONTEXT + 1), jax.random.fold_in(own_keys[1], 1), CONTEXT // 8, CONTEXT).astype(jnp.int32),
        "row_order": jax.vmap(lambda own: jax.random.permutation(own, ROWS_SET))(jax.random.split(own_keys[2], SETS)).reshape((SETS, ROWS_SET)).astype(jnp.int32),
        "lengths": plant(jax.random.randint(own_keys[3], (SHARDS,), CAP // 8, CAP + 1), jax.random.fold_in(own_keys[3], 1), CAP // 8, CAP).astype(jnp.int32),
        "cache_keys": draw_cache_keys(jax.random.fold_in(jax.random.fold_in(key_list[6], part), 71), part),
        "cache_values": bell_draw(own_keys[5], (SHARDS, KVH, CAP, HD), 1.0, 6.0, ((0, 4), (1, 2))),
    }


masked_score = -1.0e30


def combine_parts(running, latest):
    run_out, run_tot, run_top = running
    new_out, new_tot, new_top = latest
    joined = jnp.maximum(run_top, new_top)
    older = jnp.exp(run_top - joined)
    newer = jnp.exp(new_top - joined)
    return (run_out * older[..., None] + new_out * newer[..., None], run_tot * older + new_tot * newer, joined)


def reference(queries, positions, row_order, lengths, cache_keys, cache_values):
    scaling = float(HD) ** -0.5
    offsets = (jnp.cumsum(lengths) - lengths).astype(jnp.int32)
    query_all = queries.astype(jnp.float32).reshape(SETS, ROWS_SET, KVH, GQ, HD)
    initial = (jnp.zeros((SETS, ROWS_SET, KVH, GQ, HD), jnp.float32),
               jnp.zeros((SETS, ROWS_SET, KVH, GQ), jnp.float32),
               jnp.full((SETS, ROWS_SET, KVH, GQ), masked_score, jnp.float32))

    def per_shard(running, shard_data):
        key_shard, value_shard, offset, length = shard_data
        for block in range(CAP // KB):
            first_slot = block * KB
            key_block = key_shard[:, first_slot:first_slot + KB].astype(jnp.float32)
            value_block = value_shard[:, first_slot:first_slot + KB].astype(jnp.float32)
            scores = jnp.einsum("erkgd,kjd->erkgj", query_all, key_block) * scaling
            slot_ids = first_slot + jnp.arange(KB, dtype=jnp.int32)
            visible = (slot_ids < length)[None, None, :] & ((offset + slot_ids)[None, None, :] < positions[:, :, None])
            visible = visible[:, :, None, None, :]
            highest = jnp.max(jnp.where(visible, scores, masked_score), axis=-1)
            weights = jnp.where(visible, jnp.exp(scores - highest[..., None]), 0.0)
            totals = jnp.sum(weights, axis=-1)
            rounded = lax.optimization_barrier(weights.astype(jnp.bfloat16)).astype(jnp.float32)
            block_out = jnp.einsum("erkgj,kjd->erkgd", rounded, value_block)
            running = combine_parts(running, (block_out, totals, highest))
        return running, None

    final, unused = lax.scan(per_shard, initial, (cache_keys, cache_values, offsets, lengths))
    result = final[0] / final[1][..., None]
    result = result.reshape(SETS, ROWS_SET, HQ, HD)
    placed = jax.vmap(lambda chosen, indices: chosen[indices])(result, row_order.astype(jnp.int32))
    return placed.astype(jnp.bfloat16)
```

```python
import functools
import math

import jax
import jax.numpy as jnp
from jax import lax
from jax.experimental import pallas as pl
from jax.experimental.pallas import tpu as pltpu
from jax.sharding import PartitionSpec as P

KB = 256
MASKED = -1e30
FLOOR = -1e29
STEPS = 32767.0
MESH = pl.DeviceIdType.MESH


def kernel(
    n, scale,
    pos_hbm, order_hbm, len_hbm, q_hbm, k_hbm, v_hbm,
    out_ref,
    pos_all, order, len_all, q_own, q_all, k_buf, v_buf, vt_buf, sent, came, sent_stat, came_stat,
    local_sem, pos_send, pos_recv, len_send, len_recv, order_send, order_recv, q_send, q_recv,
    part_send, part_recv, stat_send, stat_recv,
):
    me = lax.axis_index("blk")
    other = 1 - lax.axis_index("beam")
    rows, kv, group, width = q_hbm.shape
    cap = k_hbm.shape[1]
    lanes = rows * group

    q_in = [pltpu.make_async_copy(q_hbm.at[:, h], q_own.at[h], local_sem.at[h]) for h in range(kv)]
    k_in = [pltpu.make_async_copy(k_hbm.at[h], k_buf.at[h], local_sem.at[kv + h]) for h in range(kv)]
    v_in = [pltpu.make_async_copy(v_hbm.at[h], v_buf.at[h], local_sem.at[2 * kv + h]) for h in range(kv)]

    barrier = pltpu.get_barrier_semaphore()
    for d in range(n):
        pl.semaphore_signal(barrier, inc=1, device_id={"blk": d, "beam": other}, device_id_type=MESH)
    for copy in q_in + v_in + k_in:
        copy.start()

    def remote(src, dst, send, recv, d):
        return pltpu.make_async_remote_copy(
            src_ref=src, dst_ref=dst, send_sem=send, recv_sem=recv,
            device_id={"blk": d, "beam": other}, device_id_type=MESH,
        )

    def pos_copy(d, source):
        return remote(pos_hbm, pos_all.at[source], pos_send.at[d], pos_recv.at[source], d)

    def len_copy(d, source):
        return remote(len_hbm, len_all.at[source], len_send.at[d], len_recv.at[source], d)

    def order_copy():
        return remote(order_hbm, order, order_send, order_recv, me)

    def q_copy(h, d, source):
        return remote(
            q_own.at[h], q_all[h].at[pl.ds(source * rows, rows)],
            q_send.at[h, d], q_recv.at[h, source], d,
        )

    def parcel(h, d, source):
        return remote(
            sent.at[h, d], came.at[h, source],
            part_send.at[h, d], part_recv.at[h, source], d,
        )

    def stat(h, d, source):
        return remote(
            sent_stat.at[h, d], came_stat.at[h, source],
            stat_send.at[h, d], stat_recv.at[h, source], d,
        )

    for h in range(kv):
        q_in[h].wait()
    pl.semaphore_wait(barrier, n)
    for d in range(n - 1, -1, -1):
        pos_copy(d, me).start()
        len_copy(d, me).start()
    order_copy().start()
    for h in range(kv):
        for d in range(n - 1, -1, -1):
            q_copy(h, d, me).start()

    for h in range(kv):
        v_in[h].wait()
        vt_buf[h] = v_buf[h].astype(jnp.float32).T.astype(jnp.bfloat16)
        k_in[h].wait()

    order_copy().wait_recv()
    for s in range(n):
        pos_copy(s, s).wait_recv()
        len_copy(s, s).wait_recv()
    length = 0
    offset = 0
    for s in range(n):
        offset = offset + jnp.where(s < me, len_all[s, 0], 0)
        length = length + jnp.where(s == me, len_all[s, 0], 0)
    lane_row = lax.broadcasted_iota(jnp.int32, (1, lanes), 1) // group
    slot_ids = lax.broadcasted_iota(jnp.int32, (KB, lanes), 0)

    def part(h, d):
        pieces = []
        limit = jnp.zeros((1, lanes), jnp.int32)
        for r in range(rows):
            row = order[0, d * rows + r]
            pieces.append(q_all[h][row])
            limit = jnp.where(lane_row == r, pos_all[row // rows, 0, row % rows], limit)
        query = jnp.concatenate(pieces, axis=0)
        limit = jnp.minimum(length, limit - offset)
        outs, tots, tops = [], [], []
        for b in range(cap // KB):
            scores = lax.dot_general(
                k_buf[h, pl.ds(b * KB, KB), :], query, (((1,), (1,)), ((), ())),
                preferred_element_type=jnp.float32,
            )
            scores = jnp.where(slot_ids < limit - b * KB, scores, MASKED)
            top = jnp.max(scores, axis=0, keepdims=True)
            weights = jnp.exp2((scores - jnp.maximum(top, FLOOR)) * scale)
            tots.append(jnp.sum(weights, axis=0, keepdims=True))
            tops.append(top)
            outs.append(
                jnp.dot(
                    vt_buf[h, :, pl.ds(b * KB, KB)], weights.astype(jnp.bfloat16),
                    preferred_element_type=jnp.float32,
                )
            )
        return merge(outs, tots, tops)

    def merge(outs, tots, tops):
        best = functools.reduce(jnp.maximum, tops)
        out = tot = 0.0
        for o, t, p in zip(outs, tots, tops):
            factor = jnp.exp2((p - best) * scale)
            out = out + o * factor
            tot = tot + t * factor
        return out, tot, best

    for h in range(kv):
        for s in range(n):
            q_copy(h, s, s).wait_recv()
        for d in range(n):
            out, tot, top = part(h, d)
            largest = jnp.max(jnp.abs(out), axis=0, keepdims=True)
            unit = jnp.where(largest > 0.0, largest, 1.0)
            sent[h, d] = jnp.round(out * (STEPS / unit)).astype(jnp.int32).astype(jnp.int16)
            sent_stat[h, d, pl.ds(0, 1), :] = tot
            sent_stat[h, d, pl.ds(1, 1), :] = top
            sent_stat[h, d, pl.ds(2, 1), :] = unit * (1.0 / STEPS)
            parcel(h, d, me).start()
            stat(h, d, me).start()

    for h in range(kv):
        outs, tots, tops = [], [], []
        for s in range(n):
            stat(h, s, s).wait_recv()
            parcel(h, s, s).wait_recv()
            unit = came_stat[h, s, pl.ds(2, 1), :]
            outs.append(came[h, s].astype(jnp.int32).astype(jnp.float32) * unit)
            tots.append(came_stat[h, s, pl.ds(0, 1), :])
            tops.append(came_stat[h, s, pl.ds(1, 1), :])
        out, tot, _ = merge(outs, tots, tops)
        out_ref[:, h] = (out / tot).T.astype(jnp.bfloat16).reshape(rows, group, width)

    order_copy().wait_send()
    for d in range(n):
        pos_copy(d, me).wait_send()
        len_copy(d, me).wait_send()
        for h in range(kv):
            q_copy(h, d, me).wait_send()
            parcel(h, d, me).wait_send()
            stat(h, d, me).wait_send()


def per_device(n, queries, positions, row_order, lengths, cache_keys, cache_values):
    keys, values = cache_keys[0], cache_values[0]
    kv, cap, width = keys.shape
    rows = queries.shape[1]
    group = queries.shape[2] // kv
    scale = float(width) ** -0.5 * math.log2(math.e)
    lanes = rows * group
    hbm = pl.BlockSpec(memory_space=pltpu.HBM)
    dma = pltpu.SemaphoreType.DMA
    out = pl.pallas_call(
        functools.partial(kernel, n, scale),
        out_shape=pltpu.VMEM((rows, kv, group, width), jnp.bfloat16),
        in_specs=[hbm] * 6,
        out_specs=pl.BlockSpec(memory_space=pltpu.VMEM),
        scratch_shapes=[
            pltpu.SMEM((n, 1, rows), jnp.int32),
            pltpu.SMEM((1, n * rows), jnp.int32),
            pltpu.SMEM((n, 1), jnp.int32),
            pltpu.VMEM((kv, rows, group, width), jnp.bfloat16),
            [pltpu.VMEM((n * rows, group, width), jnp.bfloat16) for _ in range(kv)],
            pltpu.VMEM((kv, cap, width), jnp.bfloat16),
            pltpu.VMEM((kv, cap, width), jnp.bfloat16),
            pltpu.VMEM((kv, width, cap), jnp.bfloat16),
            pltpu.VMEM((kv, n, width, lanes), jnp.int16),
            pltpu.VMEM((kv, n, width, lanes), jnp.int16),
            pltpu.VMEM((kv, n, 8, lanes), jnp.float32),
            pltpu.VMEM((kv, n, 8, lanes), jnp.float32),
            dma((3 * kv,)),
            dma((n,)), dma((n,)), dma((n,)), dma((n,)), dma(()), dma(()),
            dma((kv, n)), dma((kv, n)), dma((kv, n)), dma((kv, n)), dma((kv, n)), dma((kv, n)),
        ],
        compiler_params=pltpu.CompilerParams(collective_id=0, has_side_effects=True),
        name="attend",
    )(
        positions, row_order, lengths,
        queries.reshape(rows, kv, group, width), keys, values,
    )
    return out.reshape(queries.shape)


def solution(mesh):
    placed = (
        P(("groups", "beam"), "blk", "heads", None),
        P(("groups", "beam"), "blk"),
        P(("groups", "beam"), None),
        P(("groups", "blk")),
        P(("groups", "blk"), "heads", None, None),
        P(("groups", "blk"), "heads", None, None),
    )
    return jax.shard_map(
        functools.partial(per_device, mesh.shape["blk"]),
        mesh=mesh,
        in_specs=placed,
        out_specs=P(("groups", "beam"), "blk", "heads", None),
        check_vma=False,
    )
```

```python
import functools
import math

import jax
import jax.numpy as jnp
from jax import lax
from jax.experimental import pallas as pl
from jax.experimental.pallas import tpu as pltpu
from jax.sharding import PartitionSpec as P

KB = 256
MASKED = -1e30
FLOOR = -1e29
STEPS = 32767.0
GROUP = 4
DELAY = 2
NEAREST = 1.5 * 2.0**23


def dest_order(n):
    return sorted(range(n), key=lambda d: d)


MESH = pl.DeviceIdType.MESH


def kernel(
    n, scale,
    pos_hbm, order_hbm, len_hbm, q_hbm, k_hbm, v_hbm,
    out_ref,
    pos_all, order, len_all, q_own, q_all, k_buf, v_buf, vt_buf, sent, came, sent_stat, came_stat,
    above, q_sem, kv_sem, meta_send, meta_recv, q_send, q_recv, part_send, part_recv, stat_send, stat_recv,
):
    me = lax.axis_index("blk")
    other = 1 - lax.axis_index("beam")
    rows, kv, group, width = q_hbm.shape
    cap = k_hbm.shape[1]
    lanes = rows * group

    q_in = pltpu.make_async_copy(q_hbm, q_own, q_sem)
    k_in = pltpu.make_async_copy(k_hbm, k_buf, kv_sem.at[0])
    v_in = pltpu.make_async_copy(v_hbm, v_buf, kv_sem.at[1])

    barrier = pltpu.get_barrier_semaphore()
    for d in range(n):
        @pl.when(d >= me)
        def _():
            pl.semaphore_signal(barrier, inc=1, device_id={"blk": d, "beam": other}, device_id_type=MESH)
    q_in.start()
    v_in.start()
    k_in.start()

    def remote(src, dst, send, recv, d):
        return pltpu.make_async_remote_copy(
            src_ref=src, dst_ref=dst, send_sem=send, recv_sem=recv,
            device_id={"blk": d, "beam": other}, device_id_type=MESH,
        )

    def pos_copy(d):
        return remote(pos_hbm, pos_all.at[me], meta_send.at[0], meta_recv.at[0], d)

    def len_copy(d):
        return remote(len_hbm, len_all.at[me], meta_send.at[1], meta_recv.at[1], d)

    def order_copy():
        return remote(order_hbm, order, meta_send.at[2], meta_recv.at[2], me)

    def q_copy(h, d):
        return remote(
            q_own.at[:, h], q_all[h].at[pl.ds(me * rows, rows)], q_send.at[h], q_recv.at[h], d
        )

    def parcel(h, d):
        return remote(sent.at[h, d], came.at[h, me], part_send.at[h], part_recv.at[h], d)

    def stat(h, d):
        return remote(sent_stat.at[h, d], came_stat.at[h, me], stat_send.at[h], stat_recv.at[h], d)

    def settle(ref, semaphore):
        pltpu.make_async_copy(ref, ref, semaphore).wait()

    def first_sends(d):
        pos_copy(d).start()
        len_copy(d).start()
        q_copy(0, d).start()

    pl.semaphore_wait(barrier, me + 1)
    for d in range(n - 1):
        @pl.when(d < me)
        def _():
            pl.semaphore_signal(above.at[me], inc=1, device_id={"blk": d, "beam": other}, device_id_type=MESH)
    q_in.wait()
    order_copy().start()
    for d in range(n):
        pl.when(d <= me)(functools.partial(first_sends, d))
    for step in range(1, n):
        @pl.when(me + step < n)
        def _():
            pl.semaphore_wait(above.at[me + step], 1)
            first_sends(me + step)
    v_in.wait()
    for h in range(kv):
        vt_buf[h] = v_buf[h].astype(jnp.float32).T.astype(jnp.bfloat16)
        if h + 1 < kv:
            pl.when(other == 0)(lambda: settle(q_all[h], q_send.at[h]))
            for d in range(n):
                q_copy(h + 1, d).start()
    k_in.wait()

    order_copy().wait_recv()
    settle(pos_all, meta_recv.at[0])
    settle(len_all, meta_recv.at[1])
    length = 0
    offset = 0
    for s in range(n):
        offset = offset + jnp.where(s < me, len_all[s, 0], 0)
        length = length + jnp.where(s == me, len_all[s, 0], 0)
    lane_row = lax.broadcasted_iota(jnp.int32, (1, lanes), 1) // group
    slot_ids = lax.broadcasted_iota(jnp.int32, (KB, lanes), 0)

    blocks = cap // KB

    def gather(h, d):
        pieces = []
        limit = jnp.zeros((1, lanes), jnp.int32)
        for r in range(rows):
            row = order[0, d * rows + r]
            pieces.append(q_all[h][row])
            limit = jnp.where(lane_row == r, pos_all[row // rows, 0, row % rows], limit)
        return jnp.concatenate(pieces, axis=0), jnp.minimum(length, limit - offset)

    def dot(h, query, b):
        return lax.dot_general(
            k_buf[h, pl.ds(b * KB, KB), :], query, (((1,), (1,)), ((), ())),
            preferred_element_type=jnp.float32,
        )

    def finish(h, d, outs, tots, tops):
        best = functools.reduce(jnp.maximum, tops)
        out = tot = 0.0
        for o, t, p in zip(outs, tots, tops):
            factor = jnp.exp2((p - best) * scale)
            out = out + o * factor
            tot = tot + t * factor
        largest = jnp.max(jnp.abs(out), axis=0, keepdims=True)
        unit = jnp.where(largest > 0.0, largest, 1.0)
        sent[h, d] = (out * (STEPS / unit) + NEAREST - NEAREST).astype(jnp.int32).astype(jnp.int16)
        sent_stat[h, d, pl.ds(0, 1), :] = tot
        sent_stat[h, d, pl.ds(1, 1), :] = best
        sent_stat[h, d, pl.ds(2, 1), :] = unit * (1.0 / STEPS)

    def parts(h, dests):
        fetched = [gather(h, d) for d in dests]
        steps = [(i, b) for i in range(len(dests)) for b in range(blocks)]
        ahead = dot(h, fetched[0][0], 0)
        done = ready = None
        for at, (i, b) in enumerate(steps):
            query, limit = fetched[i]
            if b == 0:
                outs, tots, tops = [], [], []
            scores = jnp.where(slot_ids < limit - b * KB, ahead, MASKED)
            if at + 1 < len(steps):
                j, c = steps[at + 1]
                ahead = dot(h, fetched[j][0], c)
            top = jnp.max(scores, axis=0, keepdims=True)
            weights = jnp.exp2((scores - jnp.maximum(top, FLOOR)) * scale)
            tots.append(jnp.sum(weights, axis=0, keepdims=True))
            tops.append(top)
            outs.append(
                jnp.dot(
                    vt_buf[h, :, pl.ds(b * KB, KB)], weights.astype(jnp.bfloat16),
                    preferred_element_type=jnp.float32,
                )
            )
            if done is not None and b == 0:
                finish(h, *done)
                ready = done[0]
                done = None
            if ready is not None and b == DELAY:
                parcel(h, ready).start()
                stat(h, ready).start()
                ready = None
            if b + 1 == blocks:
                done = (dests[i], outs, tots, tops)
        finish(h, *done)
        parcel(h, done[0]).start()
        stat(h, done[0]).start()

    for h in range(kv):
        settle(q_all[h], q_recv.at[h])
        ordered = dest_order(n)
        for i in range(0, n, GROUP):
            dests = ordered[i:i + GROUP]
            parts(h, dests)

    settle(pos_all, meta_send.at[0])
    settle(len_all, meta_send.at[1])
    order_copy().wait_send()
    settle(q_all[kv - 1], q_send.at[kv - 1])
    for h in range(kv - 1):
        pl.when(other == 1)(lambda: settle(q_all[h], q_send.at[h]))

    for h in range(kv):
        settle(came_stat.at[h], stat_recv.at[h])
        tops = [came_stat[h, s, pl.ds(1, 1), :] for s in range(n)]
        best = functools.reduce(jnp.maximum, tops)
        factors = [jnp.exp2((p - best) * scale) for p in tops]
        tot = sum(came_stat[h, s, pl.ds(0, 1), :] * factors[s] for s in range(n))
        inverse = 1.0 / tot
        settle(came.at[h], part_recv.at[h])
        out = 0.0
        for s in range(n):
            factor = came_stat[h, s, pl.ds(2, 1), :] * factors[s] * inverse
            out = out + came[h, s].astype(jnp.int32).astype(jnp.float32) * factor
        out_ref[:, h] = out.T.astype(jnp.bfloat16).reshape(rows, group, width)

    for h in range(kv):
        settle(sent.at[h], part_send.at[h])
        settle(sent_stat.at[h], stat_send.at[h])


def per_device(n, queries, positions, row_order, lengths, cache_keys, cache_values):
    keys, values = cache_keys[0], cache_values[0]
    kv, cap, width = keys.shape
    rows = queries.shape[1]
    group = queries.shape[2] // kv
    scale = float(width) ** -0.5 * math.log2(math.e)
    lanes = rows * group
    hbm = pl.BlockSpec(memory_space=pltpu.HBM)
    dma = pltpu.SemaphoreType.DMA
    out = pl.pallas_call(
        functools.partial(kernel, n, scale),
        out_shape=pltpu.VMEM((rows, kv, group, width), jnp.bfloat16),
        in_specs=[hbm] * 6,
        out_specs=pl.BlockSpec(memory_space=pltpu.VMEM),
        scratch_shapes=[
            pltpu.SMEM((n, 1, rows), jnp.int32),
            pltpu.SMEM((1, n * rows), jnp.int32),
            pltpu.SMEM((n, 1), jnp.int32),
            pltpu.VMEM((rows, kv, group, width), jnp.bfloat16),
            [pltpu.VMEM((n * rows, group, width), jnp.bfloat16) for _ in range(kv)],
            pltpu.VMEM((kv, cap, width), jnp.bfloat16),
            pltpu.VMEM((kv, cap, width), jnp.bfloat16),
            pltpu.VMEM((kv, width, cap), jnp.bfloat16),
            pltpu.VMEM((kv, n, width, lanes), jnp.int16),
            pltpu.VMEM((kv, n, width, lanes), jnp.int16),
            pltpu.VMEM((kv, n, 3, lanes), jnp.float32),
            pltpu.VMEM((kv, n, 3, lanes), jnp.float32),
            pltpu.SemaphoreType.REGULAR((n,)),
            dma(()), dma((2,)), dma((3,)), dma((3,)),
            dma((kv,)), dma((kv,)), dma((kv,)), dma((kv,)), dma((kv,)), dma((kv,)),
        ],
        compiler_params=pltpu.CompilerParams(collective_id=0, has_side_effects=True),
        name="attend",
    )(
        positions, row_order, lengths,
        queries.reshape(rows, kv, group, width), keys, values,
    )
    return out.reshape(queries.shape)


def solution(mesh):
    placed = (
        P(("groups", "beam"), "blk", "heads", None),
        P(("groups", "beam"), "blk"),
        P(("groups", "beam"), None),
        P(("groups", "blk")),
        P(("groups", "blk"), "heads", None, None),
        P(("groups", "blk"), "heads", None, None),
    )
    return jax.shard_map(
        functools.partial(per_device, mesh.shape["blk"]),
        mesh=mesh,
        in_specs=placed,
        out_specs=P(("groups", "beam"), "blk", "heads", None),
        check_vma=False,
    )
```

```python
import functools
import math

import jax
import jax.numpy as jnp
from jax import lax
from jax.experimental import pallas as pl
from jax.experimental.pallas import tpu as pltpu
from jax.sharding import PartitionSpec as P

KB = 256
MASKED = -1e30
FLOOR = -1e29
STEPS = 32767.0
GROUP = 2
DELAY = 2
NEAREST = 1.5 * 2.0**23


def dest_order(n):
    return sorted(range(n), key=lambda d: d)


MESH = pl.DeviceIdType.MESH


def kernel(
    n, scale,
    pos_hbm, order_hbm, len_hbm, q_hbm, k_hbm, v_hbm,
    out_ref,
    pos_all, order, len_all, q_own, q_all, k_buf, v_buf, vt_buf, sent, came, sent_stat, came_stat,
    above, q_sem, kv_sem, meta_send, meta_recv, q_send, q_recv, pass_send, part_send, part_recv, stat_send, stat_recv,
):
    me = lax.axis_index("blk")
    other = 1 - lax.axis_index("beam")
    rows, kv, group, width = q_hbm.shape
    cap = k_hbm.shape[1]
    lanes = rows * group

    q_in = [pltpu.make_async_copy(q_hbm.at[r], q_own.at[r], q_sem) for r in range(rows)]
    k_in = pltpu.make_async_copy(k_hbm, k_buf, kv_sem.at[0])
    v_in = pltpu.make_async_copy(v_hbm, v_buf, kv_sem.at[1])

    folded = n > 2 and n % 2 == 0
    odd = lax.rem(me, 2)
    passer = (odd == 0) & (me > 0)
    passed = (odd == 1) & (me < n - 1)
    beside = {"blk": jnp.where(odd == 1, me - 1, me + 1)}

    barrier = pltpu.get_barrier_semaphore()
    for d in range(n):
        @pl.when((d > me) | ((d == me) & (other == 0)))
        def _():
            pl.semaphore_signal(barrier, inc=1, device_id={"blk": d, "beam": other}, device_id_type=MESH)
    if folded:
        @pl.when(passer)
        def _():
            pl.semaphore_signal(barrier, inc=1, device_id=beside, device_id_type=MESH)
    for copy in q_in:
        copy.start()
    v_in.start()
    k_in.start()

    def remote(src, dst, send, recv, d):
        return pltpu.make_async_remote_copy(
            src_ref=src, dst_ref=dst, send_sem=send, recv_sem=recv,
            device_id={"blk": d, "beam": other}, device_id_type=MESH,
        )

    def pos_copy(d):
        return remote(pos_hbm, pos_all.at[me], meta_send.at[0], meta_recv.at[0], d)

    def len_copy(d):
        return remote(len_hbm, len_all.at[me], meta_send.at[1], meta_recv.at[1], d)

    def order_copy():
        return remote(order_hbm, order, meta_send.at[2], meta_recv.at[2], me)

    def q_copy(h, d):
        onward = jnp.where((d == me + 1) & passed, 1, 0) if folded else 0
        return remote(
            q_own.at[:, h], q_all[h].at[pl.ds(me * rows, rows)], q_send.at[h], q_recv.at[onward, h], d
        )

    def send_q(h, d):
        if folded:
            pl.when(jnp.logical_not((d == me + 2) & passed))(lambda: q_copy(h, d).start())
        else:
            q_copy(h, d).start()

    def pass_copy(h):
        slot = q_all[h].at[pl.ds((me - 1) * rows, rows)]
        return pltpu.make_async_remote_copy(
            src_ref=slot, dst_ref=slot, send_sem=pass_send.at[h], recv_sem=q_recv.at[0, h],
            device_id=beside, device_id_type=MESH,
        )

    def pass_q(h):
        if folded:
            @pl.when(passer)
            def _():
                settle(q_all[h].at[pl.ds(0, rows)], q_recv.at[1, h])
                pass_copy(h).start()

    def settle_q(h, semaphore, fewer):
        if folded:
            @pl.when(fewer)
            def _():
                settle(q_all[h].at[pl.ds(0, (n - 1) * rows)], semaphore)

            @pl.when(jnp.logical_not(fewer))
            def _():
                settle(q_all[h], semaphore)
        else:
            settle(q_all[h], semaphore)

    def parcel(h, d):
        return remote(sent.at[h, d], came.at[h, me], part_send.at[h], part_recv.at[h], d)

    def stat(h, d):
        return remote(sent_stat.at[h, d], came_stat.at[h, me], stat_send.at[h], stat_recv.at[h], d)

    def settle(ref, semaphore):
        pltpu.make_async_copy(ref, ref, semaphore).wait()

    def first_sends(d):
        pos_copy(d).start()
        len_copy(d).start()
        send_q(0, d)

    greeted = me + other
    if folded:
        greeted = greeted + jnp.where((odd == 1) & (me > 1), 1, 0)

    @pl.when(greeted > 0)
    def _():
        pl.semaphore_wait(barrier, greeted)

    for d in range(n):
        @pl.when((d < me) | ((d == me) & (other == 1)))
        def _():
            pl.semaphore_signal(above.at[me], inc=1, device_id={"blk": d, "beam": other}, device_id_type=MESH)
    if folded:
        @pl.when((odd == 1) & (me > 1))
        def _():
            pl.semaphore_signal(above.at[n], inc=1, device_id=beside, device_id_type=MESH)
    settle(q_own, q_sem)
    for d in range(n - 2, -1, -1):
        pl.when((d < me) & (other == 1))(functools.partial(first_sends, d))
    for d in range(n - 1):
        pl.when((d < me) & (other == 0))(functools.partial(first_sends, d))
    pl.when(other == 0)(lambda: pl.semaphore_wait(above.at[me], 1))
    order_copy().start()
    first_sends(me)
    for step in range(1, n):
        @pl.when(me + step < n)
        def _():
            pl.semaphore_wait(above.at[me + step], 1)
            first_sends(me + step)
            if step == 1 and folded:
                for h in range(1, kv):
                    pl.when(passed)(functools.partial(send_q, h, me + step))
    v_in.wait()
    for h in range(kv):
        vt_buf[h] = v_buf[h].astype(jnp.float32).T.astype(jnp.bfloat16)
        if h + 1 < kv:
            pl.when(other == 0)(lambda: settle_q(h, q_send.at[h], passed))
            for d in range(n):
                pl.when((d > me) & jnp.logical_not(passed & (d == me + 1)))(functools.partial(send_q, h + 1, d))
            for d in range(n):
                pl.when(d <= me)(functools.partial(send_q, h + 1, d))
    k_in.wait()

    order_copy().wait_recv()
    settle(pos_all, meta_recv.at[0])
    settle(len_all, meta_recv.at[1])
    length = 0
    offset = 0
    for s in range(n):
        offset = offset + jnp.where(s < me, len_all[s, 0], 0)
        length = length + jnp.where(s == me, len_all[s, 0], 0)
    lane_row = lax.broadcasted_iota(jnp.int32, (1, lanes), 1) // group
    slot_ids = lax.broadcasted_iota(jnp.int32, (KB, lanes), 0)

    blocks = cap // KB

    def gather(h, d):
        pieces = []
        limit = jnp.zeros((1, lanes), jnp.int32)
        for r in range(rows):
            row = order[0, d * rows + r]
            pieces.append(q_all[h][row])
            limit = jnp.where(lane_row == r, pos_all[row // rows, 0, row % rows], limit)
        return jnp.concatenate(pieces, axis=0), jnp.minimum(length, limit - offset)

    def dot(h, query, b):
        return lax.dot_general(
            k_buf[h, pl.ds(b * KB, KB), :], query, (((1,), (1,)), ((), ())),
            preferred_element_type=jnp.float32,
        )

    def finish(h, d, outs, tots, tops):
        best = functools.reduce(jnp.maximum, tops)
        out = tot = 0.0
        for o, t, p in zip(outs, tots, tops):
            factor = jnp.exp2((p - best) * scale)
            out = out + o * factor
            tot = tot + t * factor
        largest = jnp.max(jnp.abs(out), axis=0, keepdims=True)
        unit = jnp.where(largest > 0.0, largest, 1.0)
        sent[h, d] = (out * (STEPS / unit) + NEAREST - NEAREST).astype(jnp.int32).astype(jnp.int16)
        sent_stat[h, d, pl.ds(0, 1), :] = tot
        sent_stat[h, d, pl.ds(1, 1), :] = best
        sent_stat[h, d, pl.ds(2, 1), :] = unit * (1.0 / STEPS)

    def parts(h, dests):
        fetched = [gather(h, d) for d in dests]
        steps = [(i, b) for i in range(len(dests)) for b in range(blocks)]
        ahead = dot(h, fetched[0][0], 0)
        done = ready = None
        for at, (i, b) in enumerate(steps):
            query, limit = fetched[i]
            if b == 0:
                outs, tots, tops = [], [], []
            scores = jnp.where(slot_ids < limit - b * KB, ahead, MASKED)
            if at + 1 < len(steps):
                j, c = steps[at + 1]
                ahead = dot(h, fetched[j][0], c)
            top = jnp.max(scores, axis=0, keepdims=True)
            weights = jnp.exp2((scores - jnp.maximum(top, FLOOR)) * scale)
            tots.append(jnp.sum(weights, axis=0, keepdims=True))
            tops.append(top)
            outs.append(
                jnp.dot(
                    vt_buf[h, :, pl.ds(b * KB, KB)], weights.astype(jnp.bfloat16),
                    preferred_element_type=jnp.float32,
                )
            )
            if done is not None and b == 0:
                finish(h, *done)
                ready = done[0]
                done = None
            if ready is not None and b == DELAY:
                parcel(h, ready).start()
                stat(h, ready).start()
                ready = None
            if b + 1 == blocks:
                done = (dests[i], outs, tots, tops)
        finish(h, *done)
        parcel(h, done[0]).start()
        stat(h, done[0]).start()

    if folded:
        pl.when(passer)(lambda: pl.semaphore_wait(above.at[n], 1))
    pass_q(0)
    for h in range(kv):
        settle_q(h, q_recv.at[0, h], passer)
        ordered = dest_order(n)
        if h + 1 < kv:
            pass_q(h + 1)
        for i in range(0, n, GROUP):
            dests = ordered[i:i + GROUP]
            parts(h, dests)

    settle(pos_all, meta_send.at[0])
    settle(len_all, meta_send.at[1])
    order_copy().wait_send()
    settle_q(kv - 1, q_send.at[kv - 1], passed)
    for h in range(kv - 1):
        pl.when(other == 1)(lambda: settle_q(h, q_send.at[h], passed))
    if folded:
        @pl.when(passer)
        def _():
            for h in range(kv):
                pass_copy(h).wait_send()

    for h in range(kv):
        settle(came_stat.at[h], stat_recv.at[h])
        tops = [came_stat[h, s, pl.ds(1, 1), :] for s in range(n)]
        best = functools.reduce(jnp.maximum, tops)
        factors = [jnp.exp2((p - best) * scale) for p in tops]
        tot = sum(came_stat[h, s, pl.ds(0, 1), :] * factors[s] for s in range(n))
        inverse = 1.0 / tot
        settle(came.at[h], part_recv.at[h])
        out = 0.0
        for s in range(n):
            factor = came_stat[h, s, pl.ds(2, 1), :] * factors[s] * inverse
            out = out + came[h, s].astype(jnp.int32).astype(jnp.float32) * factor
        out_ref[:, h] = out.T.astype(jnp.bfloat16).reshape(rows, group, width)

    for h in range(kv):
        settle(sent.at[h], part_send.at[h])
        settle(sent_stat.at[h], stat_send.at[h])


def per_device(n, queries, positions, row_order, lengths, cache_keys, cache_values):
    keys, values = cache_keys[0], cache_values[0]
    kv, cap, width = keys.shape
    rows = queries.shape[1]
    group = queries.shape[2] // kv
    scale = float(width) ** -0.5 * math.log2(math.e)
    lanes = rows * group
    hbm = pl.BlockSpec(memory_space=pltpu.HBM)
    dma = pltpu.SemaphoreType.DMA
    out = pl.pallas_call(
        functools.partial(kernel, n, scale),
        out_shape=pltpu.VMEM((rows, kv, group, width), jnp.bfloat16),
        in_specs=[hbm] * 6,
        out_specs=pl.BlockSpec(memory_space=pltpu.VMEM),
        scratch_shapes=[
            pltpu.SMEM((n, 1, rows), jnp.int32),
            pltpu.SMEM((1, n * rows), jnp.int32),
            pltpu.SMEM((n, 1), jnp.int32),
            pltpu.VMEM((rows, kv, group, width), jnp.bfloat16),
            [pltpu.VMEM((n * rows, group, width), jnp.bfloat16) for _ in range(kv)],
            pltpu.VMEM((kv, cap, width), jnp.bfloat16),
            pltpu.VMEM((kv, cap, width), jnp.bfloat16),
            pltpu.VMEM((kv, width, cap), jnp.bfloat16),
            pltpu.VMEM((kv, n, width, lanes), jnp.int16),
            pltpu.VMEM((kv, n, width, lanes), jnp.int16),
            pltpu.VMEM((kv, n, 3, lanes), jnp.float32),
            pltpu.VMEM((kv, n, 3, lanes), jnp.float32),
            pltpu.SemaphoreType.REGULAR((n + 1,)),
            dma(()), dma((2,)), dma((3,)), dma((3,)),
            dma((kv,)), dma((2, kv)), dma((kv,)), dma((kv,)), dma((kv,)), dma((kv,)), dma((kv,)),
        ],
        compiler_params=pltpu.CompilerParams(collective_id=0, has_side_effects=True),
        name="attend",
    )(
        positions, row_order, lengths,
        queries.reshape(rows, kv, group, width), keys, values,
    )
    return out.reshape(queries.shape)


def solution(mesh):
    placed = (
        P(("groups", "beam"), "blk", "heads", None),
        P(("groups", "beam"), "blk"),
        P(("groups", "beam"), None),
        P(("groups", "blk")),
        P(("groups", "blk"), "heads", None, None),
        P(("groups", "blk"), "heads", None, None),
    )
    return jax.shard_map(
        functools.partial(per_device, mesh.shape["blk"]),
        mesh=mesh,
        in_specs=placed,
        out_specs=P(("groups", "beam"), "blk", "heads", None),
        check_vma=False,
    )
```

```python
import functools
import math

import jax
import jax.numpy as jnp
from jax import lax
from jax.experimental import pallas as pl
from jax.experimental.pallas import tpu as pltpu
from jax.sharding import PartitionSpec as P

KB = 256
MASKED = -1e30
FLOOR = -1e29
STEPS = 32767.0
GROUP = 4
DELAY = 2
NEAREST = 1.5 * 2.0**23


def dest_order(n):
    return sorted(range(n), key=lambda d: d)


MESH = pl.DeviceIdType.MESH


def kernel(
    n, scale,
    pos_hbm, order_hbm, len_hbm, q_hbm, k_hbm, v_hbm,
    out_ref,
    pos_all, order, len_all, q_own, q_all, k_buf, v_buf, vt_buf, sent, came, sent_stat, came_stat,
    above, q_sem, kv_sem, meta_send, meta_recv, q_send, q_recv, part_send, part_recv, stat_send, stat_recv,
):
    me = lax.axis_index("blk")
    other = 1 - lax.axis_index("beam")
    rows, kv, group, width = q_hbm.shape
    cap = k_hbm.shape[1]
    lanes = rows * group

    q_in = pltpu.make_async_copy(q_hbm, q_own, q_sem)
    k_in = pltpu.make_async_copy(k_hbm, k_buf, kv_sem.at[0])
    v_in = pltpu.make_async_copy(v_hbm, v_buf, kv_sem.at[1])

    barrier = pltpu.get_barrier_semaphore()
    for d in range(n):
        @pl.when(d >= me)
        def _():
            pl.semaphore_signal(barrier, inc=1, device_id={"blk": d, "beam": other}, device_id_type=MESH)
    q_in.start()
    v_in.start()
    k_in.start()

    def remote(src, dst, send, recv, d):
        return pltpu.make_async_remote_copy(
            src_ref=src, dst_ref=dst, send_sem=send, recv_sem=recv,
            device_id={"blk": d, "beam": other}, device_id_type=MESH,
        )

    def pos_copy(d):
        return remote(pos_hbm, pos_all.at[me], meta_send.at[0], meta_recv.at[0], d)

    def len_copy(d):
        return remote(len_hbm, len_all.at[me], meta_send.at[1], meta_recv.at[1], d)

    def order_copy():
        return remote(order_hbm, order, meta_send.at[2], meta_recv.at[2], me)

    def q_copy(h, d):
        return remote(
            q_own.at[:, h], q_all[h].at[pl.ds(me * rows, rows)], q_send.at[h], q_recv.at[h], d
        )

    def parcel(h, d):
        return remote(sent.at[h, d], came.at[h, me], part_send.at[h], part_recv.at[h], d)

    def stat(h, d):
        return remote(sent_stat.at[h, d], came_stat.at[h, me], stat_send.at[h], stat_recv.at[h], d)

    def settle(ref, semaphore):
        pltpu.make_async_copy(ref, ref, semaphore).wait()

    def first_sends(d):
        pos_copy(d).start()
        len_copy(d).start()
        q_copy(0, d).start()

    pl.semaphore_wait(barrier, me + 1)
    for d in range(n - 1):
        @pl.when(d < me)
        def _():
            pl.semaphore_signal(above.at[me], inc=1, device_id={"blk": d, "beam": other}, device_id_type=MESH)
    q_in.wait()
    order_copy().start()
    for d in range(n - 1, -1, -1):
        pl.when(d <= me)(functools.partial(first_sends, d))
    for step in range(1, n):
        @pl.when(me + step < n)
        def _():
            pl.semaphore_wait(above.at[me + step], 1)
            first_sends(me + step)
    v_in.wait()
    for h in range(kv):
        vt_buf[h] = v_buf[h].astype(jnp.float32).T.astype(jnp.bfloat16)
        if h + 1 < kv:
            pl.when(other == 0)(lambda: settle(q_all[h], q_send.at[h]))
            for d in (*range(1, n), 0):
                q_copy(h + 1, d).start()
    k_in.wait()

    order_copy().wait_recv()
    settle(pos_all, meta_recv.at[0])
    settle(len_all, meta_recv.at[1])
    length = 0
    offset = 0
    for s in range(n):
        offset = offset + jnp.where(s < me, len_all[s, 0], 0)
        length = length + jnp.where(s == me, len_all[s, 0], 0)
    lane_row = lax.broadcasted_iota(jnp.int32, (1, lanes), 1) // group
    slot_ids = lax.broadcasted_iota(jnp.int32, (KB, lanes), 0)

    blocks = cap // KB

    def gather(h, d):
        pieces = []
        limit = jnp.zeros((1, lanes), jnp.int32)
        for r in range(rows):
            row = order[0, d * rows + r]
            pieces.append(q_all[h][row])
            limit = jnp.where(lane_row == r, pos_all[row // rows, 0, row % rows], limit)
        return jnp.concatenate(pieces, axis=0), jnp.minimum(length, limit - offset)

    def dot(h, query, b):
        return lax.dot_general(
            k_buf[h, pl.ds(b * KB, KB), :], query, (((1,), (1,)), ((), ())),
            preferred_element_type=jnp.float32,
        )

    def finish(h, d, outs, tots, tops):
        best = functools.reduce(jnp.maximum, tops)
        out = tot = 0.0
        for o, t, p in zip(outs, tots, tops):
            factor = jnp.exp2((p - best) * scale)
            out = out + o * factor
            tot = tot + t * factor
        largest = jnp.max(jnp.abs(out), axis=0, keepdims=True)
        unit = jnp.where(largest > 0.0, largest, 1.0)
        sent[h, d] = (out * (STEPS / unit) + NEAREST - NEAREST).astype(jnp.int32).astype(jnp.int16)
        sent_stat[h, d, pl.ds(0, 1), :] = tot
        sent_stat[h, d, pl.ds(1, 1), :] = best
        sent_stat[h, d, pl.ds(2, 1), :] = unit * (1.0 / STEPS)

    def parts(h, dests):
        fetched = [gather(h, d) for d in dests]
        steps = [(i, b) for i in range(len(dests)) for b in range(blocks)]
        ahead = dot(h, fetched[0][0], 0)
        done = ready = None
        for at, (i, b) in enumerate(steps):
            query, limit = fetched[i]
            if b == 0:
                outs, tots, tops = [], [], []
            scores = jnp.where(slot_ids < limit - b * KB, ahead, MASKED)
            if at + 1 < len(steps):
                j, c = steps[at + 1]
                ahead = dot(h, fetched[j][0], c)
            top = jnp.max(scores, axis=0, keepdims=True)
            weights = jnp.exp2((scores - jnp.maximum(top, FLOOR)) * scale)
            tots.append(jnp.sum(weights, axis=0, keepdims=True))
            tops.append(top)
            outs.append(
                jnp.dot(
                    vt_buf[h, :, pl.ds(b * KB, KB)], weights.astype(jnp.bfloat16),
                    preferred_element_type=jnp.float32,
                )
            )
            if done is not None and b == 0:
                finish(h, *done)
                ready = done[0]
                done = None
            if ready is not None and b == DELAY:
                parcel(h, ready).start()
                stat(h, ready).start()
                ready = None
            if b + 1 == blocks:
                done = (dests[i], outs, tots, tops)
        finish(h, *done)
        parcel(h, done[0]).start()
        stat(h, done[0]).start()

    for h in range(kv):
        settle(q_all[h], q_recv.at[h])
        ordered = dest_order(n)
        for i in range(0, n, GROUP):
            dests = ordered[i:i + GROUP]
            parts(h, dests)

    settle(pos_all, meta_send.at[0])
    settle(len_all, meta_send.at[1])
    order_copy().wait_send()
    settle(q_all[kv - 1], q_send.at[kv - 1])
    for h in range(kv - 1):
        pl.when(other == 1)(lambda: settle(q_all[h], q_send.at[h]))

    for h in range(kv):
        settle(came_stat.at[h], stat_recv.at[h])
        tops = [came_stat[h, s, pl.ds(1, 1), :] for s in range(n)]
        best = functools.reduce(jnp.maximum, tops)
        factors = [jnp.exp2((p - best) * scale) for p in tops]
        tot = sum(came_stat[h, s, pl.ds(0, 1), :] * factors[s] for s in range(n))
        inverse = 1.0 / tot
        settle(came.at[h], part_recv.at[h])
        out = 0.0
        for s in range(n):
            factor = came_stat[h, s, pl.ds(2, 1), :] * factors[s] * inverse
            out = out + came[h, s].astype(jnp.int32).astype(jnp.float32) * factor
        out_ref[:, h] = out.T.astype(jnp.bfloat16).reshape(rows, group, width)

    for h in range(kv):
        settle(sent.at[h], part_send.at[h])
        settle(sent_stat.at[h], stat_send.at[h])


def per_device(n, queries, positions, row_order, lengths, cache_keys, cache_values):
    keys, values = cache_keys[0], cache_values[0]
    kv, cap, width = keys.shape
    rows = queries.shape[1]
    group = queries.shape[2] // kv
    scale = float(width) ** -0.5 * math.log2(math.e)
    lanes = rows * group
    hbm = pl.BlockSpec(memory_space=pltpu.HBM)
    dma = pltpu.SemaphoreType.DMA
    out = pl.pallas_call(
        functools.partial(kernel, n, scale),
        out_shape=pltpu.VMEM((rows, kv, group, width), jnp.bfloat16),
        in_specs=[hbm] * 6,
        out_specs=pl.BlockSpec(memory_space=pltpu.VMEM),
        scratch_shapes=[
            pltpu.SMEM((n, 1, rows), jnp.int32),
            pltpu.SMEM((1, n * rows), jnp.int32),
            pltpu.SMEM((n, 1), jnp.int32),
            pltpu.VMEM((rows, kv, group, width), jnp.bfloat16),
            [pltpu.VMEM((n * rows, group, width), jnp.bfloat16) for _ in range(kv)],
            pltpu.VMEM((kv, cap, width), jnp.bfloat16),
            pltpu.VMEM((kv, cap, width), jnp.bfloat16),
            pltpu.VMEM((kv, width, cap), jnp.bfloat16),
            pltpu.VMEM((kv, n, width, lanes), jnp.int16),
            pltpu.VMEM((kv, n, width, lanes), jnp.int16),
            pltpu.VMEM((kv, n, 3, lanes), jnp.float32),
            pltpu.VMEM((kv, n, 3, lanes), jnp.float32),
            pltpu.SemaphoreType.REGULAR((n,)),
            dma(()), dma((2,)), dma((3,)), dma((3,)),
            dma((kv,)), dma((kv,)), dma((kv,)), dma((kv,)), dma((kv,)), dma((kv,)),
        ],
        compiler_params=pltpu.CompilerParams(collective_id=0, has_side_effects=True),
        name="attend",
    )(
        positions, row_order, lengths,
        queries.reshape(rows, kv, group, width), keys, values,
    )
    return out.reshape(queries.shape)


def solution(mesh):
    placed = (
        P(("groups", "beam"), "blk", "heads", None),
        P(("groups", "beam"), "blk"),
        P(("groups", "beam"), None),
        P(("groups", "blk")),
        P(("groups", "blk"), "heads", None, None),
        P(("groups", "blk"), "heads", None, None),
    )
    return jax.shard_map(
        functools.partial(per_device, mesh.shape["blk"]),
        mesh=mesh,
        in_specs=placed,
        out_specs=P(("groups", "beam"), "blk", "heads", None),
        check_vma=False,
    )
```

```python
import functools
import math

import jax
import jax.numpy as jnp
from jax import lax
from jax.experimental import pallas as pl
from jax.experimental.pallas import tpu as pltpu
from jax.sharding import PartitionSpec as P

KB = 256
MASKED = -1e30
FLOOR = -1e29
STEPS = 32767.0
GROUP = 4
DELAY = 2
NEAREST = 1.5 * 2.0**23


def dest_order(n):
    return sorted(range(n), key=lambda d: d)


MESH = pl.DeviceIdType.MESH


def kernel(
    n, scale,
    pos_hbm, order_hbm, len_hbm, q_hbm, k_hbm, v_hbm,
    out_ref,
    pos_all, order, len_all, q_own, q_all, k_buf, v_buf, vt_buf, sent, came, sent_stat, came_stat,
    above, q_sem, kv_sem, meta_send, meta_recv, q_send, q_recv, part_send, part_recv, stat_send, stat_recv,
):
    me = lax.axis_index("blk")
    other = 1 - lax.axis_index("beam")
    rows, kv, group, width = q_hbm.shape
    cap = k_hbm.shape[1]
    lanes = rows * group

    q_in = pltpu.make_async_copy(q_hbm, q_own, q_sem)
    k_in = pltpu.make_async_copy(k_hbm, k_buf, kv_sem.at[0])
    v_in = pltpu.make_async_copy(v_hbm, v_buf, kv_sem.at[1])

    barrier = pltpu.get_barrier_semaphore()
    for d in range(n):
        @pl.when(d >= me)
        def _():
            pl.semaphore_signal(barrier, inc=1, device_id={"blk": d, "beam": other}, device_id_type=MESH)
    q_in.start()
    v_in.start()
    k_in.start()

    def remote(src, dst, send, recv, d):
        return pltpu.make_async_remote_copy(
            src_ref=src, dst_ref=dst, send_sem=send, recv_sem=recv,
            device_id={"blk": d, "beam": other}, device_id_type=MESH,
        )

    def pos_copy(d):
        return remote(pos_hbm, pos_all.at[me], meta_send.at[0], meta_recv.at[0], d)

    def len_copy(d):
        return remote(len_hbm, len_all.at[me], meta_send.at[1], meta_recv.at[1], d)

    def order_copy():
        return remote(order_hbm, order, meta_send.at[2], meta_recv.at[2], me)

    def q_copy(h, d):
        return remote(
            q_own.at[:, h], q_all[h].at[pl.ds(me * rows, rows)], q_send.at[h], q_recv.at[h], d
        )

    def parcel(h, d):
        return remote(sent.at[h, d], came.at[h, me], part_send.at[h], part_recv.at[h], d)

    def stat(h, d):
        return remote(sent_stat.at[h, d], came_stat.at[h, me], stat_send.at[h], stat_recv.at[h], d)

    def settle(ref, semaphore):
        pltpu.make_async_copy(ref, ref, semaphore).wait()

    def first_sends(d):
        pos_copy(d).start()
        len_copy(d).start()
        q_copy(0, d).start()

    pl.semaphore_wait(barrier, me + 1)
    for d in range(n - 1):
        @pl.when(d < me)
        def _():
            pl.semaphore_signal(above.at[me], inc=1, device_id={"blk": d, "beam": other}, device_id_type=MESH)
    q_in.wait()
    order_copy().start()
    for d in range(n - 1, -1, -1):
        pl.when(d <= me)(functools.partial(first_sends, d))
    for step in range(1, n):
        @pl.when(me + step < n)
        def _():
            pl.semaphore_wait(above.at[me + step], 1)
            first_sends(me + step)
    v_in.wait()
    for h in range(kv):
        vt_buf[h] = v_buf[h].astype(jnp.float32).T.astype(jnp.bfloat16)
        if h + 1 < kv:
            pl.when(other == 0)(lambda: settle(q_all[h], q_send.at[h]))
            for d in (*range(1, n), 0):
                q_copy(h + 1, d).start()
    k_in.wait()

    order_copy().wait_recv()
    settle(pos_all, meta_recv.at[0])
    settle(len_all, meta_recv.at[1])
    length = 0
    offset = 0
    for s in range(n):
        offset = offset + jnp.where(s < me, len_all[s, 0], 0)
        length = length + jnp.where(s == me, len_all[s, 0], 0)
    lane_row = lax.broadcasted_iota(jnp.int32, (1, lanes), 1) // group
    slot_ids = lax.broadcasted_iota(jnp.int32, (KB, lanes), 0)

    blocks = cap // KB

    def gather(h, d):
        pieces = []
        limit = jnp.zeros((1, lanes), jnp.int32)
        for r in range(rows):
            row = order[0, d * rows + r]
            pieces.append(q_all[h][row])
            limit = jnp.where(lane_row == r, pos_all[row // rows, 0, row % rows], limit)
        return jnp.concatenate(pieces, axis=0), jnp.minimum(length, limit - offset)

    def dot(h, query, b):
        return lax.dot_general(
            k_buf[h, pl.ds(b * KB, KB), :], query, (((1,), (1,)), ((), ())),
            preferred_element_type=jnp.float32,
        )

    def finish(h, d, outs, tots, tops):
        best = functools.reduce(jnp.maximum, tops)
        out = tot = 0.0
        for o, t, p in zip(outs, tots, tops):
            factor = jnp.exp2((p - best) * scale)
            out = out + o * factor
            tot = tot + t * factor
        largest = jnp.max(jnp.abs(out), axis=0, keepdims=True)
        unit = jnp.where(largest > 0.0, largest, 1.0)
        sent[h, d] = (out * (STEPS / unit) + NEAREST - NEAREST).astype(jnp.int32).astype(jnp.int16)
        sent_stat[h, d, pl.ds(0, 1), :] = tot
        sent_stat[h, d, pl.ds(1, 1), :] = best
        sent_stat[h, d, pl.ds(2, 1), :] = unit * (1.0 / STEPS)

    def parts(h, dests):
        fetched = [gather(h, d) for d in dests]
        steps = [(i, b) for i in range(len(dests)) for b in range(blocks)]
        ahead = dot(h, fetched[0][0], 0)
        done = ready = None
        for at, (i, b) in enumerate(steps):
            query, limit = fetched[i]
            if b == 0:
                outs, tots, tops = [], [], []
            scores = jnp.where(slot_ids < limit - b * KB, ahead, MASKED)
            if at + 1 < len(steps):
                j, c = steps[at + 1]
                ahead = dot(h, fetched[j][0], c)
            top = jnp.max(scores, axis=0, keepdims=True)
            weights = jnp.exp2((scores - jnp.maximum(top, FLOOR)) * scale)
            tots.append(jnp.sum(weights, axis=0, keepdims=True))
            tops.append(top)
            outs.append(
                jnp.dot(
                    vt_buf[h, :, pl.ds(b * KB, KB)], weights.astype(jnp.bfloat16),
                    preferred_element_type=jnp.float32,
                )
            )
            if done is not None and b == 0:
                finish(h, *done)
                ready = done[0]
                done = None
            if ready is not None and b == DELAY:
                parcel(h, ready).start()
                stat(h, ready).start()
                ready = None
            if b + 1 == blocks:
                done = (dests[i], outs, tots, tops)
        finish(h, *done)
        parcel(h, done[0]).start()
        stat(h, done[0]).start()

    for h in range(kv):
        settle(q_all[h], q_recv.at[h])
        ordered = dest_order(n)
        if h > 0:
            ordered = sorted(ordered, key=lambda d: min(d, n - 1 - d))
        for i in range(0, n, GROUP):
            dests = ordered[i:i + GROUP]
            parts(h, dests)

    settle(pos_all, meta_send.at[0])
    settle(len_all, meta_send.at[1])
    order_copy().wait_send()
    settle(q_all[kv - 1], q_send.at[kv - 1])
    for h in range(kv - 1):
        pl.when(other == 1)(lambda: settle(q_all[h], q_send.at[h]))

    for h in range(kv):
        settle(came_stat.at[h], stat_recv.at[h])
        tops = [came_stat[h, s, pl.ds(1, 1), :] for s in range(n)]
        best = functools.reduce(jnp.maximum, tops)
        factors = [jnp.exp2((p - best) * scale) for p in tops]
        tot = sum(came_stat[h, s, pl.ds(0, 1), :] * factors[s] for s in range(n))
        inverse = 1.0 / tot
        settle(came.at[h], part_recv.at[h])
        out = 0.0
        for s in range(n):
            factor = came_stat[h, s, pl.ds(2, 1), :] * factors[s] * inverse
            out = out + came[h, s].astype(jnp.int32).astype(jnp.float32) * factor
        out_ref[:, h] = out.T.astype(jnp.bfloat16).reshape(rows, group, width)

    for h in range(kv):
        settle(sent.at[h], part_send.at[h])
        settle(sent_stat.at[h], stat_send.at[h])


def per_device(n, queries, positions, row_order, lengths, cache_keys, cache_values):
    keys, values = cache_keys[0], cache_values[0]
    kv, cap, width = keys.shape
    rows = queries.shape[1]
    group = queries.shape[2] // kv
    scale = float(width) ** -0.5 * math.log2(math.e)
    lanes = rows * group
    hbm = pl.BlockSpec(memory_space=pltpu.HBM)
    dma = pltpu.SemaphoreType.DMA
    out = pl.pallas_call(
        functools.partial(kernel, n, scale),
        out_shape=pltpu.VMEM((rows, kv, group, width), jnp.bfloat16),
        in_specs=[hbm] * 6,
        out_specs=pl.BlockSpec(memory_space=pltpu.VMEM),
        scratch_shapes=[
            pltpu.SMEM((n, 1, rows), jnp.int32),
            pltpu.SMEM((1, n * rows), jnp.int32),
            pltpu.SMEM((n, 1), jnp.int32),
            pltpu.VMEM((rows, kv, group, width), jnp.bfloat16),
            [pltpu.VMEM((n * rows, group, width), jnp.bfloat16) for _ in range(kv)],
            pltpu.VMEM((kv, cap, width), jnp.bfloat16),
            pltpu.VMEM((kv, cap, width), jnp.bfloat16),
            pltpu.VMEM((kv, width, cap), jnp.bfloat16),
            pltpu.VMEM((kv, n, width, lanes), jnp.int16),
            pltpu.VMEM((kv, n, width, lanes), jnp.int16),
            pltpu.VMEM((kv, n, 3, lanes), jnp.float32),
            pltpu.VMEM((kv, n, 3, lanes), jnp.float32),
            pltpu.SemaphoreType.REGULAR((n,)),
            dma(()), dma((2,)), dma((3,)), dma((3,)),
            dma((kv,)), dma((kv,)), dma((kv,)), dma((kv,)), dma((kv,)), dma((kv,)),
        ],
        compiler_params=pltpu.CompilerParams(collective_id=0, has_side_effects=True),
        name="attend",
    )(
        positions, row_order, lengths,
        queries.reshape(rows, kv, group, width), keys, values,
    )
    return out.reshape(queries.shape)


def solution(mesh):
    placed = (
        P(("groups", "beam"), "blk", "heads", None),
        P(("groups", "beam"), "blk"),
        P(("groups", "beam"), None),
        P(("groups", "blk")),
        P(("groups", "blk"), "heads", None, None),
        P(("groups", "blk"), "heads", None, None),
    )
    return jax.shard_map(
        functools.partial(per_device, mesh.shape["blk"]),
        mesh=mesh,
        in_specs=placed,
        out_specs=P(("groups", "beam"), "blk", "heads", None),
        check_vma=False,
    )
```
